32 devices in a mesh: row: 8 (over z, y), col: 4 (over x, core).
Axes of the slice: x: 2, y: 2, z: 4, core: 2. Of those that a mesh axis runs over, the one named last changes fastest.
Arguments:
- trailing: float32 [16384, 2048], P('row', 'col'), may hold values from -6 to 6
- pivots: int32 [3, 512], replicated, may hold values from 0 to 16383, as said below
- lower_inverse: float32 [3, 512, 512], replicated, as said below
- upper_inverse: float32 [3, 512, 512], replicated, as said below
Outputs:
- factored: float32 [16384, 2048], P('row', 'col')
The draws below stay inside these ranges and needn't reach their ends.
Inputs may be any that keep to these rules, and one draw needn't show every extreme that they name: pivots[k, j] is either k * 512 + j or a row at or past (k + 1) * 512; the rows at or past (k + 1) * 512 named in one panel are distinct. Each lower_inverse[k] is unit lower triangular. Each upper_inverse[k] is upper triangular with a positive diagonal.
All inputs are finite; a program needn't handle non-finite values.
Results may differ from the reference program's by a relative error of at most 0.0001.
Values sent between devices are 32-bit elements; how exact they have to be, the bound alone decides.
No kernel may reach another device: no remote copies, remote signals or barrier semaphores. Data moves between devices by JAX's collectives and lax.ppermute only.
A program may use at most 64 MiB of HBM per device.

```python
import math
import jax
import jax.numpy as jnp
from jax import lax

ORDER = 16384
NB = 512
PANELS = 3
WIDTH = 2048


def draw_pivots(key, part):
    columns = []
    for panel_index in range(PANELS):
        offset = panel_index * NB
        sub_key = jax.random.fold_in(key, panel_index)
        order_key, flag_key = jax.random.split(sub_key)
        far_rows = jax.random.permutation(order_key, ORDER - offset - NB)[:NB].astype(jnp.int32) + offset + NB
        flags = jax.random.randint(flag_key, (NB,), 0, 4)
        own_rows = offset + jnp.arange(NB, dtype=jnp.int32)
        columns.append(jnp.where(flags > 0, far_rows, own_rows).astype(jnp.int32))
    return jnp.stack(columns)


def draw_lower_inverse(key, part):
    normals = jax.random.normal(jax.random.fold_in(key, 11), (PANELS, NB, NB), jnp.float32)
    row_ids = jnp.arange(NB)[:, None]
    col_ids = jnp.arange(NB)[None, :]
    strict = (row_ids > col_ids)[None, :, :]
    unit = (row_ids == col_ids)[None, :, :].astype(jnp.float32)
    return (jnp.where(strict, normals / math.sqrt(NB), 0.0) + unit).astype(jnp.float32)


def draw_upper_inverse(key, part):
    normal_key, diag_key = jax.random.split(jax.random.fold_in(key, 23))
    normals = jax.random.normal(normal_key, (PANELS, NB, NB), jnp.float32)
    diag_vals = jnp.exp(jax.random.uniform(diag_key, (PANELS, NB, 1), jnp.float32, math.log(0.5), math.log(2.0)))
    row_ids = jnp.arange(NB)[:, None]
    col_ids = jnp.arange(NB)[None, :]
    strict = (row_ids < col_ids)[None, :, :]
    on_diag = (row_ids == col_ids)[None, :, :]
    values = jnp.where(strict, normals / (4.0 * NB), 0.0) + jnp.where(on_diag, diag_vals / (4.0 * math.sqrt(NB)), 0.0)
    return values.astype(jnp.float32)


def block_scale(own_key, shape, shards, low, high):
    factor_of, own = 1.0, jax.random.fold_in(own_key, 6)
    for axis_at, shards_of in shards:
        draws = jnp.exp(jax.random.uniform(jax.random.fold_in(own, axis_at), (shards_of,), jnp.float32, low / len(shards), high / len(shards)))
        factor_of = factor_of * jnp.repeat(draws, shape[axis_at] // shards_of).reshape([-1 if axis == axis_at else 1 for axis in range(len(shape))])
    return factor_of


def normal_values(stream_key, shape, scale, reach, cuts=(), kind=jnp.bfloat16):
    factor_of = block_scale(stream_key, shape, cuts, -0.22, 0.18) if cuts else 1.0
    drawn = jax.random.normal(stream_key, shape, jnp.float32) * scale * factor_of
    return jnp.minimum(jnp.maximum(drawn, -reach), reach).astype(kind)


def setup_inputs(seed: int = 0) -> dict:
    seeds = jax.random.split(jax.random.key(seed), 5)
    trailing = normal_values(seeds[0], (ORDER, WIDTH), 1.0, 6.0, ((0, 8), (1, 4)), jnp.float32)
    pivots = draw_pivots(jax.random.fold_in(seeds[4], 71), 0)
    lower_inverse = draw_lower_inverse(jax.random.fold_in(seeds[4], 71), 0)
    upper_inverse = draw_upper_inverse(jax.random.fold_in(seeds[4], 71), 0)
    return {"trailing": trailing, "pivots": pivots, "lower_inverse": lower_inverse, "upper_inverse": upper_inverse}


def reference(trailing, pivots, lower_inverse, upper_inverse):
    matrix = trailing
    for panel_index in range(PANELS):
        offset = panel_index * NB
        chosen = pivots[panel_index]
        new_top = matrix[chosen]
        old_top = matrix[offset:offset + NB]
        matrix = matrix.at[chosen].set(old_top)
        matrix = matrix.at[offset:offset + NB].set(new_top)
        upper = jnp.dot(lower_inverse[panel_index], matrix[offset:offset + NB, offset + NB:],
                        precision=lax.Precision.HIGHEST, preferred_element_type=jnp.float32)
        lower = jnp.dot(matrix[offset + NB:, offset:offset + NB], upper_inverse[panel_index],
                        precision=lax.Precision.HIGHEST, preferred_element_type=jnp.float32)
        matrix = matrix.at[offset:offset + NB, offset + NB:].set(upper)
        matrix = matrix.at[offset + NB:, offset:offset + NB].set(lower)
        update = jnp.dot(lower, upper, precision=lax.Precision.HIGHEST, preferred_element_type=jnp.float32)
        matrix = matrix.at[offset + NB:, offset + NB:].add(-update)
    return matrix
```

```python
import functools
import math
import jax
import jax.numpy as jnp
from jax import lax
from jax.experimental import pallas as pl
from jax.experimental.pallas import tpu as pltpu

from jax.sharding import PartitionSpec as P


HI = lax.Precision.HIGHEST


def dot(a, b, precision=lax.Precision.HIGH):
    return jnp.dot(a, b, precision=precision, preferred_element_type=jnp.float32)


def up8(x):
    return -(-int(x) // 8) * 8


def ring_sum(block, axis, size):
    pairs = [(i, (i + 1) % size) for i in range(size)]

    def step(_, carry):
        moving, total = carry
        moving = lax.ppermute(moving, axis, pairs)
        return moving, total + moving

    return lax.fori_loop(0, size - 1, step, (block, block))[1]


def plain_steps(matrix, pivots, lower_inverse, upper_inverse, total):
    row_count, col_count = matrix.shape
    panel_count, block_size = pivots.shape
    row_place = lax.axis_index("row")
    col_place = lax.axis_index("col")
    row_ids = row_place * row_count + jnp.arange(row_count, dtype=jnp.int32)
    col_ids = col_place * col_count + jnp.arange(col_count, dtype=jnp.int32)

    def panel_step(panel, matrix):
        offset = panel * block_size
        chosen = pivots[panel]
        local_index = chosen - row_place * row_count
        is_owned = (local_index >= 0) & (local_index < row_count)
        picked = jnp.take(matrix, jnp.clip(local_index, 0, row_count - 1), axis=0)
        picked = jnp.where(is_owned[:, None], picked, 0.0)
        top_device = offset // row_count
        top_start = offset % row_count
        top = lax.dynamic_slice_in_dim(matrix, top_start, block_size, 0)
        top = jnp.where(row_place == top_device, top, 0.0)
        both = total(jnp.concatenate([picked, top]), "row")
        gathered, displaced = both[:block_size], both[block_size:]
        beyond = col_ids >= offset + block_size
        solved = dot(lower_inverse[panel], gathered, HI)
        new_top = jnp.where(beyond[None, :], solved, gathered)
        matches = row_ids[:, None] == chosen[None, :]
        hit_rows = jnp.any(matches, axis=1)
        source = jnp.argmax(matches, axis=1)
        matrix = jnp.where(hit_rows[:, None], jnp.take(displaced, source, axis=0), matrix)
        placed = lax.dynamic_update_slice_in_dim(matrix, new_top, top_start, 0)
        matrix = jnp.where(row_place == top_device, placed, matrix)
        panel_device = offset // col_count
        below = (row_ids >= offset + block_size)[:, None]
        factor = jnp.where(below, dot(matrix, upper_inverse[panel], HI), matrix)
        factor = total(jnp.where(col_place == panel_device, factor, 0.0), "col")
        matrix = jnp.where(col_place == panel_device, factor, matrix)
        left = jnp.where(below, factor, 0.0)
        right = jnp.where(beyond[None, :], new_top, 0.0)
        return matrix - dot(left, right, HI)

    return lax.fori_loop(0, panel_count, panel_step, matrix)


def ranks(owner, live, nr):
    n = owner.shape[1]
    hot = ((owner[:, :, None] == jnp.arange(nr)) & live[:, :, None]).astype(jnp.bfloat16)
    before = (jnp.arange(n)[:, None] > jnp.arange(n)[None, :]).astype(jnp.bfloat16)
    rank = jnp.einsum("ij,kjd->kid", before, hot, preferred_element_type=jnp.float32)
    own_rank = jnp.sum(rank * hot.astype(jnp.float32), axis=2).astype(jnp.int32)
    counts = jnp.sum(hot.astype(jnp.float32), axis=1).astype(jnp.int32)
    return own_rank, counts


def pick(hot, values):
    return jnp.sum(jnp.where(hot, values[..., None, :], 0), axis=-1)


def plan(pivots, row_count, nr, caps):
    cx, cb, ce, cd = caps
    K, n = pivots.shape
    place = lax.axis_index("row")

    def lookup(p, upto):
        res = p
        for kk in range(upto):
            eq = p[:, None] == pivots[kk][None, :]
            val = jnp.sum(jnp.where(eq, old[kk][None, :] + 1, 0), axis=1)
            res = jnp.where(val > 0, val - 1, res)
        return res

    old, new = [], []
    for k in range(K):
        both = lookup(jnp.concatenate([k * n + jnp.arange(n, dtype=jnp.int32), pivots[k]]), k)
        old.append(both[:n])
        new.append(both[n:])
    old, new = jnp.stack(old), jnp.stack(new)

    owner = new // row_count
    slot, counts = ranks(owner, jnp.ones(owner.shape, bool), nr)
    roomy = jnp.where(jnp.arange(K) == 0, cx + cb, cx + nr * ce)[:, None]
    fits = jnp.all(counts <= jnp.where(jnp.arange(nr)[None, :] == 0, roomy, cx))
    local = new - owner * row_count
    hot = (owner == place)[:, None, :] & (slot[:, None, :] == jnp.arange(cx)[None, :, None])
    take_x = pick(hot, local)
    extra = jnp.where(owner == 0, slot - cx, -1)
    take_b = pick(extra[0][None, :] == jnp.arange(cb)[:, None], local[0])
    hot = extra[1:, None, :] == jnp.arange(nr * ce)[None, :, None]
    take_e = pick(hot, local[1:]).reshape(K - 1, nr, ce).transpose(1, 0, 2)
    first = (jnp.arange(K) == 0)[:, None]
    home = jnp.where((extra < 0) | first, owner, extra // ce)
    away = home ^ place
    piece = (away % 2) * (nr // 2) + away // 2
    within = jnp.where(extra < 0, slot, cx + extra % ce)
    select = piece * jnp.where(first, cx, cx + ce) + within
    select = jnp.where(first & (extra >= 0), nr * cx + extra, select)
    select = jnp.clip(select, 0, nr * cx + jnp.where(first, cb, nr * ce) - 1)

    live = pivots >= K * n
    for k in range(K):
        for kk in range(k + 1, K):
            again = jnp.any(pivots[k][:, None] == pivots[kk][None, :], axis=1)
            live = live.at[k].set(live[k] & ~again)
    dest = pivots // row_count
    dslot, dcounts = ranks(dest, live, nr)
    start = jnp.cumsum(dcounts, axis=0) - dcounts
    dhot = dest[:, :, None] == jnp.arange(nr)
    dslot = dslot + jnp.sum(jnp.where(dhot, start[:, None, :], 0), axis=2)
    fits = fits & jnp.all(jnp.sum(dcounts, axis=0) <= cd)
    flat = jnp.where(live & (dslot < cd), dest * cd + dslot, -1).reshape(-1)
    dhot = flat[None, :] == jnp.arange(nr * cd)[:, None]
    take_d = pick(dhot, old.reshape(-1))
    mine = flat - place * cd
    mhot = mine[None, :] == jnp.arange(cd)[:, None]
    put_d = pick(mhot, pivots.reshape(-1) + 1) - 1 - place * row_count
    return fits, take_x, take_b, take_e, select, take_d, put_d


def parts(a):
    high = a.astype(jnp.bfloat16)
    return high, (a - high.astype(jnp.float32)).astype(jnp.bfloat16)


def dot3(a, b):
    f = functools.partial(jnp.dot, preferred_element_type=jnp.float32)
    return f(a[0], b[0]) + (f(a[0], b[1]) + f(a[1], b[0]))


KEEP, SUBTRACT, REPLACE = 0, 1, 2
VM = pl.BlockSpec(memory_space=pltpu.VMEM)
SM = pl.BlockSpec(memory_space=pltpu.SMEM)


def limit(*rows):
    return pltpu.CompilerParams(vmem_limit_bytes=sum(rows) * 2048 + 4 * 2**20)


def rows_kernel(tile, starts, lefts, has_inverse, has_out, flags, *refs):
    refs = list(refs)
    sources = [refs.pop(0) for _ in starts]
    left_refs = [refs.pop(0) for _ in lefts]
    upper_ref = refs.pop(0) if lefts else None
    inverse_ref = refs.pop(0) if has_inverse else None
    out_ref = refs.pop(0) if has_out else None
    next_ref = refs.pop(0) if has_inverse else None
    mode, which, solve = flags[0], flags[1], flags[2]
    if lefts:
        upper, refs = refs[:2], refs[2:]

        @pl.when(mode == SUBTRACT)
        def _():
            upper[0][...], upper[1][...] = parts(upper_ref[...])

    if has_inverse:
        inverse = refs[:2]

        @pl.when(solve == 1)
        def _():
            inverse[0][...], inverse[1][...] = parts(inverse_ref[...])

    done = 0
    for (start, count), source in zip(starts, sources):

        @pl.loop(0, count // tile)
        def _(i, done=done, start=start, source=source):
            into = pl.ds(pl.multiple_of(done + i * tile, 8), tile)
            rows = pl.ds(pl.multiple_of(start + i * tile, 8), tile)
            if has_out:

                @pl.when(mode == KEEP)
                def _():
                    out_ref[into, :] = source[rows, :]

                for j, (left_ref, first) in enumerate(zip(left_refs, lefts)):
                    mine = pl.ds(pl.multiple_of(first + done + i * tile, 8), tile)

                    @pl.when((mode == SUBTRACT) & (which == j))
                    def _():
                        left = parts(left_ref[mine, :])
                        out_ref[into, :] = source[rows, :] - dot3(left, (upper[0][...], upper[1][...]))

                    @pl.when((mode == REPLACE) & (which == j))
                    def _():
                        out_ref[into, :] = left_ref[mine, :]

            if has_inverse:
                here, at = (out_ref, into) if has_out else (source, rows)

                @pl.when(solve == 1)
                def _():
                    next_ref[into, :] = dot3(parts(here[at, :]), (inverse[0][...], inverse[1][...]))

        done += count


def call_rows(flags, sources, lefts=(), upper=None, inverse=None, out=True):
    n = sources[0][0].shape[1]
    rows = sum(count for _, _, count in sources)
    tile = tile_of(math.gcd(*[count for _, _, count in sources]))
    whole = [w for w in (upper, inverse) if w is not None]
    outs = int(out) + int(inverse is not None)
    return pl.pallas_call(
        functools.partial(
            rows_kernel, tile, [s[1:] for s in sources], [left[1] for left in lefts], inverse is not None, out
        ),
        out_shape=[jax.ShapeDtypeStruct((rows, n), jnp.float32)] * outs,
        in_specs=[SM] + [VM] * (len(sources) + len(lefts) + len(whole)),
        out_specs=[VM] * outs,
        scratch_shapes=[pltpu.VMEM((n, n), jnp.bfloat16)] * (2 * len(whole)),
        compiler_params=limit(*[a[0].shape[0] for a in [*sources, *lefts]], outs * rows, 2 * n * len(whole)),
        cost_estimate=pl.CostEstimate(flops=6 * rows * n * n, bytes_accessed=12 * rows * n, transcendentals=0),
    )(flags, *[s[0] for s in sources], *[s[0] for s in lefts], *whole)


def tile_of(rows):
    return max(t for t in range(8, 257, 8) if rows % t == 0)


def finish_kernel(put, first, *refs):
    out_ref = refs[-1]
    bodies, moved_ref, tops = refs[:2], refs[2], refs[3:-1]
    start = 0
    for body in bodies:
        size = min(body.shape[0], out_ref.shape[0] - start)
        out_ref[start : start + size, :] = body[:size, :]
        start += size

    @pl.loop(0, moved_ref.shape[0])
    def _(s):
        at = put[s]

        @pl.when(at >= 0)
        def _():
            out_ref[pl.ds(at, 1), :] = moved_ref[pl.ds(s, 1), :]

    @pl.when(first[0] == 1)
    def _():
        for i, top in enumerate(tops):
            n = top.shape[0]
            out_ref[i * n : (i + 1) * n, :] = top[...]


def finish(put, first, bodies, moved, tops, row_count):
    return pl.pallas_call(
        finish_kernel,
        name="finish",
        out_shape=jax.ShapeDtypeStruct((row_count, moved.shape[1]), jnp.float32),
        in_specs=[SM, SM] + [VM] * (len(bodies) + 1 + len(tops)),
        out_specs=VM,
        compiler_params=limit(*[a.shape[0] for a in [*bodies, moved, *tops]], row_count),
        cost_estimate=pl.CostEstimate(flops=10**6, bytes_accessed=12 * row_count * moved.shape[1], transcendentals=0),
    )(put, first, *bodies, moved, *tops)


def top_kernel(sel, beyond, *refs):
    pools, inverse_ref, top_ref, upper_ref, pool, rows = refs[:-5], refs[-5], refs[-4], refs[-3], refs[-2], refs[-1]
    n = rows.shape[0]
    if len(pools) > 1:
        start = 0
        for part in pools:
            pool[start : start + part.shape[0], :] = part[...]
            start += part.shape[0]
    else:
        pool = pools[0]

    @pl.loop(0, n // 8)
    def _(i):
        for r in range(8):
            j = i * 8 + r
            rows[pl.ds(j, 1), :] = pool[pl.ds(sel[j], 1), :]

    upper_ref[...] = dot3(parts(inverse_ref[...]), parts(rows[...]))

    @pl.when(beyond[0] == 1)
    def _():
        top_ref[...] = upper_ref[...]

    @pl.when(beyond[0] == 0)
    def _():
        top_ref[...] = rows[...]


def call_top(sel, beyond, pools, inverse):
    n = inverse.shape[0]
    return pl.pallas_call(
        top_kernel,
        name="top",
        out_shape=[jax.ShapeDtypeStruct((n, pools[0].shape[1]), jnp.float32)] * 2,
        in_specs=[SM, SM] + [VM] * (len(pools) + 1),
        out_specs=[VM, VM],
        scratch_shapes=[
            pltpu.VMEM((sum(p.shape[0] for p in pools) if len(pools) > 1 else 8, pools[0].shape[1]), jnp.float32),
            pltpu.VMEM((n, pools[0].shape[1]), jnp.float32),
        ],
        compiler_params=limit(2 * sum(p.shape[0] for p in pools), 4 * n),
        cost_estimate=pl.CostEstimate(flops=6 * n**3, bytes_accessed=24 * n * n, transcendentals=0),
    )(sel, beyond, *pools, inverse)


def take_rows(array, index):
    return array.at[index].get(mode="clip")


def fast_steps(trailing, pivots, lower_inverse, upper_inverse, nr, nc, caps):
    cx, _, ce, cd = caps
    row_count, _ = trailing.shape
    K, n = pivots.shape
    row = lax.axis_index("row")
    col = lax.axis_index("col")
    chips = nc // 2

    def spread(left, k):
        copies = [left]
        for chip in range(k // 2 + 1, chips):
            there = 2 * chip + k % 2
            moved = lax.ppermute(left, "col", [(k, there)])
            copies += [moved, lax.ppermute(moved, "col", [(there, there ^ 1)])]
        if k ^ 1 > k:
            copies.append(lax.ppermute(left, "col", [(k, k ^ 1)]))
        return copies

    def flags(k):
        mode = jnp.where(col == k, REPLACE, jnp.where(col > k, SUBTRACT, KEEP))
        which = spread_places(k)
        return jnp.stack([mode, which, (col == k + 1).astype(jnp.int32)]).astype(jnp.int32)

    def spread_places(k):
        count, which = 1, jnp.where(col == k, 0, -1)
        if k < 0:
            return which
        for chip in range(k // 2 + 1, chips):
            there = 2 * chip + k % 2
            which = jnp.where(col == there, count, jnp.where(col == there ^ 1, count + 1, which))
            count += 2
        if k ^ 1 > k:
            which = jnp.where(col == k ^ 1, count, which)
            count += 1
        return which

    def gather(part, k, extra=None):
        pools = [part]
        for s in range(2, nr, 2):
            pools.append(lax.ppermute(part, "row", [(i, i ^ s) for i in range(nr)]))
        for pool in pools[:]:
            pools.append(lax.ppermute(pool, "row", [(r, r ^ 1) for r in range(nr)]))
        if extra is not None:
            pools.append(extra)
        return call_top(select[k], (col > k).astype(jnp.int32).reshape(1), pools, lower_inverse[k])

    def tree(rows, count):
        step = nr // 2
        while step:
            part = rows[step * count :] if count else rows
            moved = lax.ppermute(part, "row", [(i, i + step) for i in range(0, nr, 2 * step)])
            rows = jnp.where(row % (2 * step) == step, moved, rows[: step * count] if count else rows)
            step //= 2
        return rows

    half = row_count // 2
    lower_half, upper_half = trailing[:half], trailing[half:]
    flag = flags(-1)
    solve = lambda rows: call_rows(flag, [(rows, 0, rows.shape[0])], inverse=upper_inverse[0], out=False)[0]
    copies_a = spread(solve(lower_half), 0)
    copies_b = spread(solve(upper_half), 0)

    fits, take_x, take_b, take_e, select, take_d, put_d = plan(pivots, row_count, nr, caps)
    own = [take_rows(trailing, take_x[0])]
    extra = tree(take_rows(trailing, take_b), 0)
    top, upper = gather(own[0], 0, extra)
    own += [take_rows(trailing, take_x[k]) for k in range(1, K)]
    width = cx + ce
    dealt = tree(take_rows(trailing, take_e.reshape(-1)), (K - 1) * ce)
    later = []
    for k in range(1, K):
        later += [own[k], dealt[(k - 1) * ce : k * ce]]
    later = jnp.concatenate(later)
    late = later.shape[0]
    solved = solve(later)
    copies_l = spread(solved, 0)

    moving = take_rows(trailing[: K * n], take_d)
    mine = moving[:cd]
    for d in range(1, nr):
        moved = lax.ppermute(moving[d * cd : (d + 1) * cd], "row", [(0, d)])
        mine = jnp.where(row == d, moved, mine)
    moving = mine
    copies_d = spread(solve(moving), 0)

    groups = {"A": lower_half, "B": upper_half, "D": moving}
    lefts = {
        "X": [(c, 0, late) for c in copies_l],
        "A": [(c, 0, half) for c in copies_a],
        "B": [(c, 0, half) for c in copies_b],
        "D": [(c, 0, cd) for c in copies_d],
    }
    tops = []
    for k in range(K):
        if k:
            top, upper = gather(part, k)
        tops.append(top)
        flag = flags(k)
        inverse = upper_inverse[k + 1] if k + 1 < K else None
        if k + 1 < K:
            count = later.shape[0]
            later, solved = call_rows(flag, [(later, 0, count)], lefts["X"], upper, inverse)
            rest = (K - 1 - k) * width
            part, later = later[:width], later[width:rest]
            if k + 2 < K:
                copies = spread(solved[width:rest], k + 1)
                lefts["X"] = [(c, 0, rest - width) for c in copies]
        for name in "ABD":
            count = groups[name].shape[0]
            res = call_rows(flag, [(groups[name], 0, count)], lefts[name], upper, inverse)
            groups[name] = res[0]
            if k + 1 < K:
                copies = spread(res[1], k + 1)
                lefts[name] = [(c, 0, count) for c in copies]
    first = (row == 0).astype(jnp.int32).reshape(1)
    return fits, finish(put_d, first, [groups["A"], groups["B"]], groups["D"], tops, row_count)


def capacities(n, nr, K):
    unit = n // nr
    cx = up8(1.15 * unit)
    ce = -(-up8(0.36 * unit) // 8) * 8
    return cx, up8(2.5 * unit), ce, up8(0.13 * K * n)


def shards(nr, nc, trailing, pivots, lower_inverse, upper_inverse):
    row_count, col_count = trailing.shape
    K, n = pivots.shape
    fits_shape = (
        K * n < row_count and nr == 8 and nc % 2 == 0 and K <= nc and n == col_count and n % (8 * nr) == 0 and row_count % 16 == 0
    )
    if not fits_shape:
        return plain_steps(trailing, pivots, lower_inverse, upper_inverse, lax.psum)
    caps = CAPS or capacities(n, nr, K)
    fits, done = fast_steps(trailing, pivots, lower_inverse, upper_inverse, nr, nc, caps)
    sizes = {"row": nr, "col": nc}

    def plain(carry):
        total = lambda block, axis: ring_sum(block, axis, sizes[axis])
        return jnp.bool_(False), plain_steps(trailing, pivots, lower_inverse, upper_inverse, total)

    return lax.while_loop(lambda carry: carry[0], plain, (~fits, done))[1]


CAPS = None


def solution(mesh):
    nr, nc = mesh.shape["row"], mesh.shape["col"]
    in_specs = (P("row", "col"), P(), P(), P())
    return jax.shard_map(
        functools.partial(shards, nr, nc), mesh=mesh, in_specs=in_specs, out_specs=P("row", "col"), check_vma=False
    )
```

```python
import functools
import math
import jax
import jax.numpy as jnp
from jax import lax
from jax.experimental import pallas as pl
from jax.experimental.pallas import tpu as pltpu

from jax.sharding import PartitionSpec as P


HI = lax.Precision.HIGHEST


def dot(a, b, precision=lax.Precision.HIGH):
    return jnp.dot(a, b, precision=precision, preferred_element_type=jnp.float32)


def up8(x):
    return -(-int(x) // 8) * 8


def ring_sum(block, axis, size):
    pairs = [(i, (i + 1) % size) for i in range(size)]

    def step(_, carry):
        moving, total = carry
        moving = lax.ppermute(moving, axis, pairs)
        return moving, total + moving

    return lax.fori_loop(0, size - 1, step, (block, block))[1]


def plain_steps(matrix, pivots, lower_inverse, upper_inverse, total):
    row_count, col_count = matrix.shape
    panel_count, block_size = pivots.shape
    row_place = lax.axis_index("row")
    col_place = lax.axis_index("col")
    row_ids = row_place * row_count + jnp.arange(row_count, dtype=jnp.int32)
    col_ids = col_place * col_count + jnp.arange(col_count, dtype=jnp.int32)

    def panel_step(panel, matrix):
        offset = panel * block_size
        chosen = pivots[panel]
        local_index = chosen - row_place * row_count
        is_owned = (local_index >= 0) & (local_index < row_count)
        picked = jnp.take(matrix, jnp.clip(local_index, 0, row_count - 1), axis=0)
        picked = jnp.where(is_owned[:, None], picked, 0.0)
        top_device = offset // row_count
        top_start = offset % row_count
        top = lax.dynamic_slice_in_dim(matrix, top_start, block_size, 0)
        top = jnp.where(row_place == top_device, top, 0.0)
        both = total(jnp.concatenate([picked, top]), "row")
        gathered, displaced = both[:block_size], both[block_size:]
        beyond = col_ids >= offset + block_size
        solved = dot(lower_inverse[panel], gathered, HI)
        new_top = jnp.where(beyond[None, :], solved, gathered)
        matches = row_ids[:, None] == chosen[None, :]
        hit_rows = jnp.any(matches, axis=1)
        source = jnp.argmax(matches, axis=1)
        matrix = jnp.where(hit_rows[:, None], jnp.take(displaced, source, axis=0), matrix)
        placed = lax.dynamic_update_slice_in_dim(matrix, new_top, top_start, 0)
        matrix = jnp.where(row_place == top_device, placed, matrix)
        panel_device = offset // col_count
        below = (row_ids >= offset + block_size)[:, None]
        factor = jnp.where(below, dot(matrix, upper_inverse[panel], HI), matrix)
        factor = total(jnp.where(col_place == panel_device, factor, 0.0), "col")
        matrix = jnp.where(col_place == panel_device, factor, matrix)
        left = jnp.where(below, factor, 0.0)
        right = jnp.where(beyond[None, :], new_top, 0.0)
        return matrix - dot(left, right, HI)

    return lax.fori_loop(0, panel_count, panel_step, matrix)


def ranks(owner, live, nr):
    n = owner.shape[1]
    hot = ((owner[:, :, None] == jnp.arange(nr)) & live[:, :, None]).astype(jnp.bfloat16)
    before = (jnp.arange(n)[:, None] > jnp.arange(n)[None, :]).astype(jnp.bfloat16)
    rank = jnp.einsum("ij,kjd->kid", before, hot, preferred_element_type=jnp.float32)
    own_rank = jnp.sum(rank * hot.astype(jnp.float32), axis=2).astype(jnp.int32)
    counts = jnp.sum(hot.astype(jnp.float32), axis=1).astype(jnp.int32)
    return own_rank, counts


def pick(hot, values):
    return jnp.sum(jnp.where(hot, values[..., None, :], 0), axis=-1)


def plan(pivots, row_count, nr, caps):
    cx, cb, ce, cd = caps
    K, n = pivots.shape
    place = lax.axis_index("row")

    def lookup(p, upto):
        res = p
        for kk in range(upto):
            eq = p[:, None] == pivots[kk][None, :]
            val = jnp.sum(jnp.where(eq, old[kk][None, :] + 1, 0), axis=1)
            res = jnp.where(val > 0, val - 1, res)
        return res

    old, new = [], []
    for k in range(K):
        both = lookup(jnp.concatenate([k * n + jnp.arange(n, dtype=jnp.int32), pivots[k]]), k)
        old.append(both[:n])
        new.append(both[n:])
    old, new = jnp.stack(old), jnp.stack(new)

    owner = new // row_count
    slot, counts = ranks(owner, jnp.ones(owner.shape, bool), nr)
    roomy = jnp.where(jnp.arange(K) == 0, cx + cb, cx + nr * ce)[:, None]
    fits = jnp.all(counts <= jnp.where(jnp.arange(nr)[None, :] == 0, roomy, cx))
    local = new - owner * row_count
    hot = (owner == place)[:, None, :] & (slot[:, None, :] == jnp.arange(cx)[None, :, None])
    take_x = pick(hot, local)
    extra = jnp.where(owner == 0, slot - cx, -1)
    take_b = pick(extra[0][None, :] == jnp.arange(cb)[:, None], local[0])
    hot = extra[1:, None, :] == jnp.arange(nr * ce)[None, :, None]
    take_e = pick(hot, local[1:]).reshape(K - 1, nr, ce).transpose(1, 0, 2)
    first = (jnp.arange(K) == 0)[:, None]
    home = jnp.where((extra < 0) | first, owner, extra // ce)
    away = home ^ place
    piece = (away % 2) * (nr // 2) + away // 2
    within = jnp.where(extra < 0, slot, cx + extra % ce)
    select = piece * jnp.where(first, cx, cx + ce) + within
    select = jnp.where(first & (extra >= 0), nr * cx + extra, select)
    select = jnp.clip(select, 0, nr * cx + jnp.where(first, cb, nr * ce) - 1)

    live = pivots >= K * n
    for k in range(K):
        for kk in range(k + 1, K):
            again = jnp.any(pivots[k][:, None] == pivots[kk][None, :], axis=1)
            live = live.at[k].set(live[k] & ~again)
    dest = pivots // row_count
    dslot, dcounts = ranks(dest, live, nr)
    start = jnp.cumsum(dcounts, axis=0) - dcounts
    dhot = dest[:, :, None] == jnp.arange(nr)
    dslot = dslot + jnp.sum(jnp.where(dhot, start[:, None, :], 0), axis=2)
    fits = fits & jnp.all(jnp.sum(dcounts, axis=0) <= cd)
    flat = jnp.where(live & (dslot < cd), dest * cd + dslot, -1).reshape(-1)
    dhot = flat[None, :] == jnp.arange(nr * cd)[:, None]
    take_d = pick(dhot, old.reshape(-1))
    mine = flat - place * cd
    mhot = mine[None, :] == jnp.arange(cd)[:, None]
    put_d = pick(mhot, pivots.reshape(-1) + 1) - 1 - place * row_count
    return fits, take_x, take_b, take_e, select, take_d, put_d


def parts(a):
    high = a.astype(jnp.bfloat16)
    return high, (a - high.astype(jnp.float32)).astype(jnp.bfloat16)


def dot3(a, b):
    f = functools.partial(jnp.dot, preferred_element_type=jnp.float32)
    return f(a[0], b[0]) + (f(a[0], b[1]) + f(a[1], b[0]))


KEEP, SUBTRACT, REPLACE = 0, 1, 2
VM = pl.BlockSpec(memory_space=pltpu.VMEM)
SM = pl.BlockSpec(memory_space=pltpu.SMEM)


def limit(*rows):
    return pltpu.CompilerParams(vmem_limit_bytes=sum(rows) * 2048 + 4 * 2**20)


def rows_kernel(tile, panel, starts, lefts, has_out, flags, *refs):
    refs = list(refs)
    sources = [refs.pop(0) for _ in starts]
    left_refs = [refs.pop(0) for _ in lefts]
    upper_ref = refs.pop(0) if lefts else None
    inverse_ref = refs.pop(0) if panel is not None else None
    out_ref = refs.pop(0) if has_out else None
    next_ref = refs.pop(0) if panel is not None else None
    sems = refs.pop()
    mode, which, solve = flags[0], flags[1], flags[2]
    rows_in = refs.pop(0)
    count = sum(c for _, c in starts)
    tiles = count // tile
    if has_out:
        fetch_rows, fetch_left = mode != REPLACE, (mode != KEEP)
    else:
        fetch_rows, fetch_left = solve == 1, None

    def source_copy(i):
        done = 0
        for source, (start, c) in zip(sources, starts):
            if i * tile < done + c:
                at = start + i * tile - done
                return pltpu.make_async_copy(
                    source.at[pl.ds(at, tile)], rows_in.at[pl.ds(i * tile, tile)], sems.at[0, i]
                )
            done += c

    def left_copy(j, i):
        return pltpu.make_async_copy(
            left_refs[j].at[pl.ds(lefts[j] + i * tile, tile)], left_in.at[pl.ds(i * tile, tile)], sems.at[1, i]
        )

    if panel is not None:
        inverse_in, inverse = refs.pop(0), [refs.pop(0), refs.pop(0)]
        inverse_copy = pltpu.make_async_copy(inverse_ref.at[panel], inverse_in, sems.at[2, 0])

        @pl.when(solve == 1)
        def _():
            inverse_copy.start()

    if lefts:
        left_in, upper = refs.pop(0), [refs.pop(0), refs.pop(0)]

    @pl.when(fetch_rows)
    def _():
        for i in range(tiles):
            source_copy(i).start()

    for j in range(len(lefts)):

        @pl.when(fetch_left & (which == j))
        def _():
            for i in range(tiles):
                left_copy(j, i).start()

    if lefts:

        @pl.when(mode == SUBTRACT)
        def _():
            upper[0][...], upper[1][...] = parts(upper_ref[...])

    if panel is not None:

        @pl.when(solve == 1)
        def _():
            inverse_copy.wait()
            inverse[0][...], inverse[1][...] = parts(inverse_in[...])

    for i in range(tiles):
        at = pl.ds(i * tile, tile)

        @pl.when(fetch_rows)
        def _():
            source_copy(i).wait()

        if lefts:

            @pl.when(fetch_left)
            def _():
                left_copy(0, i).wait()

            @pl.when(mode == KEEP)
            def _():
                out_ref[at, :] = rows_in[at, :]

            @pl.when(mode == SUBTRACT)
            def _():
                left = parts(left_in[at, :])
                out_ref[at, :] = rows_in[at, :] - dot3(left, (upper[0][...], upper[1][...]))

            @pl.when(mode == REPLACE)
            def _():
                out_ref[at, :] = left_in[at, :]

        if panel is not None:
            here = out_ref if has_out else rows_in

            @pl.when(solve == 1)
            def _():
                next_ref[at, :] = dot3(parts(here[at, :]), (inverse[0][...], inverse[1][...]))


HB = pl.BlockSpec(memory_space=pltpu.MemorySpace.HBM)


def call_rows(flags, sources, lefts=(), upper=None, inverse=None, panel=None, out=True):
    n = sources[0][0].shape[1]
    rows = sum(count for _, _, count in sources)
    tile = tile_of(math.gcd(*[count for _, _, count in sources]))
    whole = [w for w in (upper, inverse) if w is not None]
    outs = int(out) + int(inverse is not None)
    scratch = [pltpu.VMEM((rows, n), jnp.float32)]
    halves = [pltpu.VMEM((n, n), jnp.bfloat16)] * 2
    if inverse is not None:
        scratch += [pltpu.VMEM((n, n), jnp.float32)] + halves
    if lefts:
        scratch += [pltpu.VMEM((rows, n), jnp.float32)] + halves
    scratch += [pltpu.SemaphoreType.DMA((3, rows // tile))]
    return pl.pallas_call(
        functools.partial(
            rows_kernel, tile, panel, [s[1:] for s in sources], [left[1] for left in lefts], out
        ),
        out_shape=[jax.ShapeDtypeStruct((rows, n), jnp.float32)] * outs,
        in_specs=[SM]
        + [HB] * (len(sources) + len(lefts))
        + [VM] * (upper is not None)
        + [HB] * (inverse is not None),
        out_specs=[VM] * outs,
        scratch_shapes=scratch,
        compiler_params=limit((outs + 2) * rows, 6 * n),
        cost_estimate=pl.CostEstimate(flops=6 * rows * n * n, bytes_accessed=12 * rows * n, transcendentals=0),
    )(flags, *[s[0] for s in sources], *[s[0] for s in lefts], *whole)


def tile_of(rows):
    return max(t for t in range(8, 257, 8) if rows % t == 0)


def finish_kernel(put, first, *refs):
    out_ref = refs[-1]
    bodies, moved_ref, tops = refs[:2], refs[2], refs[3:-1]
    start = 0
    for body in bodies:
        size = min(body.shape[0], out_ref.shape[0] - start)
        out_ref[start : start + size, :] = body[:size, :]
        start += size

    @pl.loop(0, moved_ref.shape[0])
    def _(s):
        at = put[s]

        @pl.when(at >= 0)
        def _():
            out_ref[pl.ds(at, 1), :] = moved_ref[pl.ds(s, 1), :]

    @pl.when(first[0] == 1)
    def _():
        for i, top in enumerate(tops):
            n = top.shape[0]
            out_ref[i * n : (i + 1) * n, :] = top[...]


def finish(put, first, bodies, moved, tops, row_count):
    return pl.pallas_call(
        finish_kernel,
        name="finish",
        out_shape=jax.ShapeDtypeStruct((row_count, moved.shape[1]), jnp.float32),
        in_specs=[SM, SM] + [VM] * (len(bodies) + 1 + len(tops)),
        out_specs=VM,
        compiler_params=limit(*[a.shape[0] for a in [*bodies, moved, *tops]], row_count),
        cost_estimate=pl.CostEstimate(flops=10**6, bytes_accessed=12 * row_count * moved.shape[1], transcendentals=0),
    )(put, first, *bodies, moved, *tops)


def top_kernel(sel, beyond, *refs):
    pools, inverse_ref, top_ref, upper_ref, pool, rows = refs[:-5], refs[-5], refs[-4], refs[-3], refs[-2], refs[-1]
    n = rows.shape[0]
    if len(pools) > 1:
        start = 0
        for part in pools:
            pool[start : start + part.shape[0], :] = part[...]
            start += part.shape[0]
    else:
        pool = pools[0]

    @pl.loop(0, n // 8)
    def _(i):
        for r in range(8):
            j = i * 8 + r
            rows[pl.ds(j, 1), :] = pool[pl.ds(sel[j], 1), :]

    upper_ref[...] = dot3(parts(inverse_ref[...]), parts(rows[...]))

    @pl.when(beyond[0] == 1)
    def _():
        top_ref[...] = upper_ref[...]

    @pl.when(beyond[0] == 0)
    def _():
        top_ref[...] = rows[...]


def call_top(sel, beyond, pools, inverse):
    n = inverse.shape[0]
    return pl.pallas_call(
        top_kernel,
        name="top",
        out_shape=[jax.ShapeDtypeStruct((n, pools[0].shape[1]), jnp.float32)] * 2,
        in_specs=[SM, SM] + [VM] * (len(pools) + 1),
        out_specs=[VM, VM],
        scratch_shapes=[
            pltpu.VMEM((sum(p.shape[0] for p in pools) if len(pools) > 1 else 8, pools[0].shape[1]), jnp.float32),
            pltpu.VMEM((n, pools[0].shape[1]), jnp.float32),
        ],
        compiler_params=limit(2 * sum(p.shape[0] for p in pools), 4 * n),
        cost_estimate=pl.CostEstimate(flops=6 * n**3, bytes_accessed=24 * n * n, transcendentals=0),
    )(sel, beyond, *pools, inverse)


def take_rows(array, index):
    return array.at[index].get(mode="clip")


def fast_steps(trailing, pivots, lower_inverse, upper_inverse, nr, nc, caps):
    cx, _, ce, cd = caps
    row_count, _ = trailing.shape
    K, _ = pivots.shape
    row = lax.axis_index("row")
    col = lax.axis_index("col")
    chips = nc // 2

    def spread(left, k):
        copies = [left]
        for chip in range(k // 2 + 1, chips):
            there = 2 * chip + k % 2
            moved = lax.ppermute(left, "col", [(k, there)])
            copies += [moved, lax.ppermute(moved, "col", [(there, there ^ 1)])]
        if k ^ 1 > k:
            copies.append(lax.ppermute(left, "col", [(k, k ^ 1)]))
        return copies

    def flags(k):
        mode = jnp.where(col == k, REPLACE, jnp.where(col > k, SUBTRACT, KEEP))
        which = spread_places(k)
        return jnp.stack([mode, which, (col == k + 1).astype(jnp.int32)]).astype(jnp.int32)

    def spread_places(k):
        count, which = 1, jnp.where(col == k, 0, -1)
        if k < 0:
            return which
        for chip in range(k // 2 + 1, chips):
            there = 2 * chip + k % 2
            which = jnp.where(col == there, count, jnp.where(col == there ^ 1, count + 1, which))
            count += 2
        if k ^ 1 > k:
            which = jnp.where(col == k ^ 1, count, which)
            count += 1
        return which

    def gather(part, k, extra=None):
        pools = [part]
        for s in range(2, nr, 2):
            pools.append(lax.ppermute(part, "row", [(i, i ^ s) for i in range(nr)]))
        for pool in pools[:]:
            pools.append(lax.ppermute(pool, "row", [(r, r ^ 1) for r in range(nr)]))
        if extra is not None:
            pools.append(extra)
        return call_top(select[k], (col > k).astype(jnp.int32).reshape(1), pools, lower_inverse[k])

    def tree(rows, count):
        step = nr // 2
        while step:
            part = rows[step * count :] if count else rows
            moved = lax.ppermute(part, "row", [(i, i + step) for i in range(0, nr, 2 * step)])
            rows = jnp.where(row % (2 * step) == step, moved, rows[: step * count] if count else rows)
            step //= 2
        return rows

    half = row_count // 2
    flag = flags(-1)
    solve = lambda *source: call_rows(flag, [source], inverse=upper_inverse, panel=0, out=False)[0]
    copies_a = spread(solve(trailing, 0, half), 0)
    copies_b = spread(solve(trailing, half, half), 0)

    fits, take_x, take_b, take_e, select, take_d, put_d = plan(pivots, row_count, nr, caps)
    own = [take_rows(trailing, take_x[0])]
    extra = tree(take_rows(trailing, take_b), 0)
    top, upper = gather(own[0], 0, extra)
    own += [take_rows(trailing, take_x[k]) for k in range(1, K)]
    width = cx + ce
    dealt = tree(take_rows(trailing, take_e.reshape(-1)), (K - 1) * ce)
    later = []
    for k in range(1, K):
        later += [own[k], dealt[(k - 1) * ce : k * ce]]
    later = jnp.concatenate(later)
    late = later.shape[0]
    solved = solve(later, 0, late)
    copies_l = spread(solved, 0)

    moving = take_rows(trailing, take_d)
    mine = moving[:cd]
    for d in range(1, nr):
        moved = lax.ppermute(moving[d * cd : (d + 1) * cd], "row", [(0, d)])
        mine = jnp.where(row == d, moved, mine)
    moving = mine
    copies_d = spread(solve(moving, 0, cd), 0)

    groups = {"A": (trailing, 0, half), "B": (trailing, half, half), "D": (moving, 0, cd)}
    lefts = {
        "X": [(c, 0, late) for c in copies_l],
        "A": [(c, 0, half) for c in copies_a],
        "B": [(c, 0, half) for c in copies_b],
        "D": [(c, 0, cd) for c in copies_d],
    }
    tops = []
    for k in range(K):
        if k:
            top, upper = gather(part, k)
        tops.append(top)
        flag = flags(k)
        solving = dict(inverse=upper_inverse, panel=k + 1) if k + 1 < K else {}
        if k + 1 < K:
            count = later.shape[0]
            later, solved = call_rows(flag, [(later, 0, count)], lefts["X"], upper, **solving)
            rest = (K - 1 - k) * width
            part, later = later[:width], later[width:rest]
            if k + 2 < K:
                copies = spread(solved[width:rest], k + 1)
                lefts["X"] = [(c, 0, rest - width) for c in copies]
        for name in "ABD":
            count = groups[name][2]
            res = call_rows(flag, [groups[name]], lefts[name], upper, **solving)
            groups[name] = (res[0], 0, count)
            if k + 1 < K:
                copies = spread(res[1], k + 1)
                lefts[name] = [(c, 0, count) for c in copies]
    first = (row == 0).astype(jnp.int32).reshape(1)
    return fits, finish(put_d, first, [groups["A"][0], groups["B"][0]], groups["D"][0], tops, row_count)


def capacities(n, nr, K):
    unit = n // nr
    cx = up8(1.15 * unit)
    ce = -(-up8(0.36 * unit) // 8) * 8
    return cx, up8(2.5 * unit), ce, up8(0.13 * K * n)


def shards(nr, nc, trailing, pivots, lower_inverse, upper_inverse):
    row_count, col_count = trailing.shape
    K, n = pivots.shape
    fits_shape = (
        K * n < row_count and nr == 8 and nc % 2 == 0 and K <= nc and n == col_count and n % (8 * nr) == 0 and row_count % 16 == 0
    )
    if not fits_shape:
        return plain_steps(trailing, pivots, lower_inverse, upper_inverse, lax.psum)
    caps = CAPS or capacities(n, nr, K)
    fits, done = fast_steps(trailing, pivots, lower_inverse, upper_inverse, nr, nc, caps)
    sizes = {"row": nr, "col": nc}

    def plain(carry):
        total = lambda block, axis: ring_sum(block, axis, sizes[axis])
        return jnp.bool_(False), plain_steps(trailing, pivots, lower_inverse, upper_inverse, total)

    return lax.while_loop(lambda carry: carry[0], plain, (~fits, done))[1]


CAPS = None


def solution(mesh):
    nr, nc = mesh.shape["row"], mesh.shape["col"]
    in_specs = (P("row", "col"), P(), P(), P())
    return jax.shard_map(
        functools.partial(shards, nr, nc), mesh=mesh, in_specs=in_specs, out_specs=P("row", "col"), check_vma=False
    )
```

```python
import functools
import math
import jax
import jax.numpy as jnp
from jax import lax
from jax.experimental import pallas as pl
from jax.experimental.pallas import tpu as pltpu

from jax.sharding import PartitionSpec as P


HI = lax.Precision.HIGHEST


def dot(a, b, precision=lax.Precision.HIGH):
    return jnp.dot(a, b, precision=precision, preferred_element_type=jnp.float32)


def up8(x):
    return -(-int(x) // 8) * 8


def ring_sum(block, axis, size):
    pairs = [(i, (i + 1) % size) for i in range(size)]

    def step(_, carry):
        moving, total = carry
        moving = lax.ppermute(moving, axis, pairs)
        return moving, total + moving

    return lax.fori_loop(0, size - 1, step, (block, block))[1]


def plain_steps(matrix, pivots, lower_inverse, upper_inverse, total):
    row_count, col_count = matrix.shape
    panel_count, block_size = pivots.shape
    row_place = lax.axis_index("row")
    col_place = lax.axis_index("col")
    row_ids = row_place * row_count + jnp.arange(row_count, dtype=jnp.int32)
    col_ids = col_place * col_count + jnp.arange(col_count, dtype=jnp.int32)

    def panel_step(panel, matrix):
        offset = panel * block_size
        chosen = pivots[panel]
        local_index = chosen - row_place * row_count
        is_owned = (local_index >= 0) & (local_index < row_count)
        picked = jnp.take(matrix, jnp.clip(local_index, 0, row_count - 1), axis=0)
        picked = jnp.where(is_owned[:, None], picked, 0.0)
        top_device = offset // row_count
        top_start = offset % row_count
        top = lax.dynamic_slice_in_dim(matrix, top_start, block_size, 0)
        top = jnp.where(row_place == top_device, top, 0.0)
        both = total(jnp.concatenate([picked, top]), "row")
        gathered, displaced = both[:block_size], both[block_size:]
        beyond = col_ids >= offset + block_size
        solved = dot(lower_inverse[panel], gathered, HI)
        new_top = jnp.where(beyond[None, :], solved, gathered)
        matches = row_ids[:, None] == chosen[None, :]
        hit_rows = jnp.any(matches, axis=1)
        source = jnp.argmax(matches, axis=1)
        matrix = jnp.where(hit_rows[:, None], jnp.take(displaced, source, axis=0), matrix)
        placed = lax.dynamic_update_slice_in_dim(matrix, new_top, top_start, 0)
        matrix = jnp.where(row_place == top_device, placed, matrix)
        panel_device = offset // col_count
        below = (row_ids >= offset + block_size)[:, None]
        factor = jnp.where(below, dot(matrix, upper_inverse[panel], HI), matrix)
        factor = total(jnp.where(col_place == panel_device, factor, 0.0), "col")
        matrix = jnp.where(col_place == panel_device, factor, matrix)
        left = jnp.where(below, factor, 0.0)
        right = jnp.where(beyond[None, :], new_top, 0.0)
        return matrix - dot(left, right, HI)

    return lax.fori_loop(0, panel_count, panel_step, matrix)


def ranks(owner, live, nr):
    n = owner.shape[1]
    hot = ((owner[:, :, None] == jnp.arange(nr)) & live[:, :, None]).astype(jnp.bfloat16)
    before = (jnp.arange(n)[:, None] > jnp.arange(n)[None, :]).astype(jnp.bfloat16)
    rank = jnp.einsum("ij,kjd->kid", before, hot, preferred_element_type=jnp.float32)
    own_rank = jnp.sum(rank * hot.astype(jnp.float32), axis=2).astype(jnp.int32)
    counts = jnp.sum(hot.astype(jnp.float32), axis=1).astype(jnp.int32)
    return own_rank, counts


def pick(hot, values):
    return jnp.sum(jnp.where(hot, values[..., None, :], 0), axis=-1)


def plan(pivots, row_count, nr, caps):
    cx, cb, ce, cd = caps
    K, n = pivots.shape
    place = lax.axis_index("row")

    def lookup(p, upto):
        res = p
        for kk in range(upto):
            eq = p[:, None] == pivots[kk][None, :]
            val = jnp.sum(jnp.where(eq, old[kk][None, :] + 1, 0), axis=1)
            res = jnp.where(val > 0, val - 1, res)
        return res

    old, new = [], []
    for k in range(K):
        both = lookup(jnp.concatenate([k * n + jnp.arange(n, dtype=jnp.int32), pivots[k]]), k)
        old.append(both[:n])
        new.append(both[n:])
    old, new = jnp.stack(old), jnp.stack(new)

    owner = new // row_count
    slot, counts = ranks(owner, jnp.ones(owner.shape, bool), nr)
    roomy = jnp.where(jnp.arange(K) == 0, cx + cb, cx + nr * ce)[:, None]
    fits = jnp.all(counts <= jnp.where(jnp.arange(nr)[None, :] == 0, roomy, cx))
    local = new - owner * row_count
    hot = (owner == place)[:, None, :] & (slot[:, None, :] == jnp.arange(cx)[None, :, None])
    take_x = pick(hot, local)
    extra = jnp.where(owner == 0, slot - cx, -1)
    take_b = pick(extra[0][None, :] == jnp.arange(cb)[:, None], local[0])
    hot = extra[1:, None, :] == jnp.arange(nr * ce)[None, :, None]
    take_e = pick(hot, local[1:]).reshape(K - 1, nr, ce).transpose(1, 0, 2)
    first = (jnp.arange(K) == 0)[:, None]
    home = jnp.where((extra < 0) | first, owner, extra // ce)
    away = home ^ place
    piece = (away % 2) * (nr // 2) + away // 2
    within = jnp.where(extra < 0, slot, cx + extra % ce)
    select = piece * jnp.where(first, cx, cx + ce) + within
    select = jnp.where(first & (extra >= 0), nr * cx + extra, select)
    select = jnp.clip(select, 0, nr * cx + jnp.where(first, cb, nr * ce) - 1)

    live = pivots >= K * n
    for k in range(K):
        for kk in range(k + 1, K):
            again = jnp.any(pivots[k][:, None] == pivots[kk][None, :], axis=1)
            live = live.at[k].set(live[k] & ~again)
    dest = pivots // row_count
    dslot, dcounts = ranks(dest, live, nr)
    start = jnp.cumsum(dcounts, axis=0) - dcounts
    dhot = dest[:, :, None] == jnp.arange(nr)
    dslot = dslot + jnp.sum(jnp.where(dhot, start[:, None, :], 0), axis=2)
    fits = fits & jnp.all(jnp.sum(dcounts, axis=0) <= cd)
    flat = jnp.where(live & (dslot < cd), dest * cd + dslot, -1).reshape(-1)
    dhot = flat[None, :] == jnp.arange(nr * cd)[:, None]
    take_d = pick(dhot, old.reshape(-1))
    mine = flat - place * cd
    mhot = mine[None, :] == jnp.arange(cd)[:, None]
    put_d = pick(mhot, pivots.reshape(-1) + 1) - 1 - place * row_count
    return fits, take_x, take_b, take_e, select, take_d, put_d


def parts(a):
    high = a.astype(jnp.bfloat16)
    return high, (a - high.astype(jnp.float32)).astype(jnp.bfloat16)


def dot3(a, b):
    f = functools.partial(jnp.dot, preferred_element_type=jnp.float32)
    return f(a[0], b[0]) + (f(a[0], b[1]) + f(a[1], b[0]))


KEEP, SUBTRACT, REPLACE = 0, 1, 2
VM = pl.BlockSpec(memory_space=pltpu.VMEM)
SM = pl.BlockSpec(memory_space=pltpu.SMEM)


def limit(*rows):
    return pltpu.CompilerParams(vmem_limit_bytes=sum(rows) * 2048 + 4 * 2**20)


def rows_kernel(tile, panel, starts, lefts, has_out, flags, *refs):
    refs = list(refs)
    sources = [refs.pop(0) for _ in starts]
    left_refs = [refs.pop(0) for _ in lefts]
    upper_ref = refs.pop(0) if lefts else None
    inverse_ref = refs.pop(0) if panel is not None else None
    out_ref = refs.pop(0) if has_out else None
    next_ref = refs.pop(0) if panel is not None else None
    sems = refs.pop()
    mode, which, solve = flags[0], flags[1], flags[2]
    rows_in = refs.pop(0)
    count = sum(c for _, c in starts)
    tiles = count // tile
    if has_out:
        fetch_rows, fetch_left = mode != REPLACE, (mode != KEEP)
    else:
        fetch_rows, fetch_left = solve == 1, None

    (source,), ((first, _),) = sources, starts

    def source_copy(i):
        at = pl.ds(pl.multiple_of(first + i * tile, 8), tile)
        return pltpu.make_async_copy(source.at[at], rows_in.at[pl.ds(pl.multiple_of(i * tile, 8), tile)], sems.at[0, i])

    def left_copy(j, i):
        return pltpu.make_async_copy(
            left_refs[j].at[pl.ds(pl.multiple_of(lefts[j] + i * tile, 8), tile)],
            left_in.at[pl.ds(pl.multiple_of(i * tile, 8), tile)],
            sems.at[1, i],
        )

    if panel is not None:
        inverse_in, inverse = refs.pop(0), [refs.pop(0), refs.pop(0)]
        inverse_copy = pltpu.make_async_copy(inverse_ref.at[panel], inverse_in, sems.at[2, 0])

        @pl.when(solve == 1)
        def _():
            inverse_copy.start()

    if lefts:
        left_in, upper = refs.pop(0), [refs.pop(0), refs.pop(0)]

    @pl.when(fetch_rows)
    def _():
        for i in range(tiles):
            source_copy(i).start()

    for j in range(len(lefts)):

        @pl.when(fetch_left & (which == j))
        def _():
            for i in range(tiles):
                left_copy(j, i).start()

    if lefts:

        @pl.when(mode == SUBTRACT)
        def _():
            upper[0][...], upper[1][...] = parts(upper_ref[...])

    if panel is not None:

        @pl.when(solve == 1)
        def _():
            inverse_copy.wait()
            inverse[0][...], inverse[1][...] = parts(inverse_in[...])

    @pl.loop(0, tiles)
    def _(i):
        at = pl.ds(pl.multiple_of(i * tile, 8), tile)

        @pl.when(fetch_rows)
        def _():
            source_copy(i).wait()

        if lefts:

            @pl.when(fetch_left)
            def _():
                left_copy(0, i).wait()

            @pl.when(mode == KEEP)
            def _():
                out_ref[at, :] = rows_in[at, :]

            @pl.when(mode == SUBTRACT)
            def _():
                left = parts(left_in[at, :])
                out_ref[at, :] = rows_in[at, :] - dot3(left, (upper[0][...], upper[1][...]))

            @pl.when(mode == REPLACE)
            def _():
                out_ref[at, :] = left_in[at, :]

        if panel is not None:
            here = out_ref if has_out else rows_in

            @pl.when(solve == 1)
            def _():
                next_ref[at, :] = dot3(parts(here[at, :]), (inverse[0][...], inverse[1][...]))


HB = pl.BlockSpec(memory_space=pltpu.MemorySpace.HBM)


def call_rows(flags, sources, lefts=(), upper=None, inverse=None, panel=None, out=True):
    n = sources[0][0].shape[1]
    rows = sum(count for _, _, count in sources)
    tile = tile_of(math.gcd(*[count for _, _, count in sources]))
    whole = [w for w in (upper, inverse) if w is not None]
    outs = int(out) + int(inverse is not None)
    scratch = [pltpu.VMEM((rows, n), jnp.float32)]
    halves = [pltpu.VMEM((n, n), jnp.bfloat16)] * 2
    if inverse is not None:
        scratch += [pltpu.VMEM((n, n), jnp.float32)] + halves
    if lefts:
        scratch += [pltpu.VMEM((rows, n), jnp.float32)] + halves
    scratch += [pltpu.SemaphoreType.DMA((3, rows // tile))]
    return pl.pallas_call(
        functools.partial(
            rows_kernel, tile, panel, [s[1:] for s in sources], [left[1] for left in lefts], out
        ),
        out_shape=[jax.ShapeDtypeStruct((rows, n), jnp.float32)] * outs,
        in_specs=[SM]
        + [HB] * (len(sources) + len(lefts))
        + [VM] * (upper is not None)
        + [HB] * (inverse is not None),
        out_specs=[VM] * outs,
        scratch_shapes=scratch,
        compiler_params=limit((outs + 2) * rows, 6 * n),
        cost_estimate=pl.CostEstimate(flops=6 * rows * n * n, bytes_accessed=12 * rows * n, transcendentals=0),
    )(flags, *[s[0] for s in sources], *[s[0] for s in lefts], *whole)


def tile_of(rows):
    return max(t for t in range(8, 257, 8) if rows % t == 0)


def finish_kernel(put, first, *refs):
    out_ref = refs[-1]
    bodies, moved_ref, tops = refs[:2], refs[2], refs[3:-1]
    start = 0
    for body in bodies:
        size = min(body.shape[0], out_ref.shape[0] - start)
        out_ref[start : start + size, :] = body[:size, :]
        start += size

    @pl.loop(0, moved_ref.shape[0])
    def _(s):
        at = put[s]

        @pl.when(at >= 0)
        def _():
            out_ref[pl.ds(at, 1), :] = moved_ref[pl.ds(s, 1), :]

    @pl.when(first[0] == 1)
    def _():
        for i, top in enumerate(tops):
            n = top.shape[0]
            out_ref[i * n : (i + 1) * n, :] = top[...]


def finish(put, first, bodies, moved, tops, row_count):
    return pl.pallas_call(
        finish_kernel,
        name="finish",
        out_shape=jax.ShapeDtypeStruct((row_count, moved.shape[1]), jnp.float32),
        in_specs=[SM, SM] + [VM] * (len(bodies) + 1 + len(tops)),
        out_specs=VM,
        compiler_params=limit(*[a.shape[0] for a in [*bodies, moved, *tops]], row_count),
        cost_estimate=pl.CostEstimate(flops=10**6, bytes_accessed=12 * row_count * moved.shape[1], transcendentals=0),
    )(put, first, *bodies, moved, *tops)


def top_kernel(panel, sel, beyond, *refs):
    pools, inverse_ref, top_ref, upper_ref, pool, rows, inverse, sem = refs[:-7], *refs[-7:]
    n = rows.shape[0]
    fetch = pltpu.make_async_copy(inverse_ref.at[panel], inverse, sem)
    fetch.start()
    if len(pools) > 1:
        start = 0
        for part in pools:
            pool[start : start + part.shape[0], :] = part[...]
            start += part.shape[0]
    else:
        pool = pools[0]

    @pl.loop(0, n // 8)
    def _(i):
        for r in range(8):
            j = i * 8 + r
            rows[pl.ds(j, 1), :] = pool[pl.ds(sel[j], 1), :]

    fetch.wait()
    upper_ref[...] = dot3(parts(inverse[...]), parts(rows[...]))

    @pl.when(beyond[0] == 1)
    def _():
        top_ref[...] = upper_ref[...]

    @pl.when(beyond[0] == 0)
    def _():
        top_ref[...] = rows[...]


def call_top(sel, beyond, pools, inverse, panel):
    n = inverse.shape[1]
    return pl.pallas_call(
        functools.partial(top_kernel, panel),
        name="top",
        out_shape=[jax.ShapeDtypeStruct((n, pools[0].shape[1]), jnp.float32)] * 2,
        in_specs=[SM, SM] + [VM] * len(pools) + [HB],
        out_specs=[VM, VM],
        scratch_shapes=[
            pltpu.VMEM((sum(p.shape[0] for p in pools) if len(pools) > 1 else 8, pools[0].shape[1]), jnp.float32),
            pltpu.VMEM((n, pools[0].shape[1]), jnp.float32),
            pltpu.VMEM((n, n), jnp.float32),
            pltpu.SemaphoreType.DMA,
        ],
        compiler_params=limit(2 * sum(p.shape[0] for p in pools), 5 * n),
        cost_estimate=pl.CostEstimate(flops=6 * n**3, bytes_accessed=24 * n * n, transcendentals=0),
    )(sel, beyond, *pools, inverse)


def take_rows(array, index):
    return array.at[index].get(mode="clip")


def fast_steps(trailing, pivots, lower_inverse, upper_inverse, nr, nc, caps):
    cx, _, ce, cd = caps
    row_count, _ = trailing.shape
    K, _ = pivots.shape
    row = lax.axis_index("row")
    col = lax.axis_index("col")
    chips = nc // 2

    def spread(left, k):
        copies = [left]
        for chip in range(k // 2 + 1, chips):
            there = 2 * chip + k % 2
            moved = lax.ppermute(left, "col", [(k, there)])
            copies += [moved, lax.ppermute(moved, "col", [(there, there ^ 1)])]
        if k ^ 1 > k:
            copies.append(lax.ppermute(left, "col", [(k, k ^ 1)]))
        return copies

    def flags(k):
        mode = jnp.where(col == k, REPLACE, jnp.where(col > k, SUBTRACT, KEEP))
        which = spread_places(k)
        return jnp.stack([mode, which, (col == k + 1).astype(jnp.int32)]).astype(jnp.int32)

    def spread_places(k):
        count, which = 1, jnp.where(col == k, 0, -1)
        if k < 0:
            return which
        for chip in range(k // 2 + 1, chips):
            there = 2 * chip + k % 2
            which = jnp.where(col == there, count, jnp.where(col == there ^ 1, count + 1, which))
            count += 2
        if k ^ 1 > k:
            which = jnp.where(col == k ^ 1, count, which)
            count += 1
        return which

    def gather(part, k, extra=None):
        pools = [part]
        for s in range(2, nr, 2):
            pools.append(lax.ppermute(part, "row", [(i, i ^ s) for i in range(nr)]))
        for pool in pools[:]:
            pools.append(lax.ppermute(pool, "row", [(r, r ^ 1) for r in range(nr)]))
        if extra is not None:
            pools.append(extra)
        return call_top(select[k], (col > k).astype(jnp.int32).reshape(1), pools, lower_inverse, k)

    def tree(rows, count):
        step = nr // 2
        while step:
            part = rows[step * count :] if count else rows
            moved = lax.ppermute(part, "row", [(i, i + step) for i in range(0, nr, 2 * step)])
            rows = jnp.where(row % (2 * step) == step, moved, rows[: step * count] if count else rows)
            step //= 2
        return rows

    half = row_count // 2
    flag = flags(-1)
    solve = lambda *source: call_rows(flag, [source], inverse=upper_inverse, panel=0, out=False)[0]
    copies_a = spread(solve(trailing, 0, half), 0)
    copies_b = spread(solve(trailing, half, half), 0)

    fits, take_x, take_b, take_e, select, take_d, put_d = plan(pivots, row_count, nr, caps)
    own = [take_rows(trailing, take_x[0])]
    extra = tree(take_rows(trailing, take_b), 0)
    top, upper = gather(own[0], 0, extra)
    own += [take_rows(trailing, take_x[k]) for k in range(1, K)]
    width = cx + ce
    dealt = tree(take_rows(trailing, take_e.reshape(-1)), (K - 1) * ce)
    later = []
    for k in range(1, K):
        later += [own[k], dealt[(k - 1) * ce : k * ce]]
    later = jnp.concatenate(later)
    late = later.shape[0]
    solved = solve(later, 0, late)
    copies_l = spread(solved, 0)

    moving = take_rows(trailing, take_d)
    mine = moving[:cd]
    for d in range(1, nr):
        moved = lax.ppermute(moving[d * cd : (d + 1) * cd], "row", [(0, d)])
        mine = jnp.where(row == d, moved, mine)
    moving = mine
    copies_d = spread(solve(moving, 0, cd), 0)

    groups = {"A": (trailing, 0, half), "B": (trailing, half, half), "D": (moving, 0, cd)}
    lefts = {
        "X": [(c, 0, late) for c in copies_l],
        "A": [(c, 0, half) for c in copies_a],
        "B": [(c, 0, half) for c in copies_b],
        "D": [(c, 0, cd) for c in copies_d],
    }
    tops = []
    for k in range(K):
        if k:
            top, upper = gather(part, k)
        tops.append(top)
        flag = flags(k)
        solving = dict(inverse=upper_inverse, panel=k + 1) if k + 1 < K else {}
        if k + 1 < K:
            count = later.shape[0]
            later, solved = call_rows(flag, [(later, 0, count)], lefts["X"], upper, **solving)
            rest = (K - 1 - k) * width
            part, later = later[:width], later[width:rest]
            if k + 2 < K:
                copies = spread(solved[width:rest], k + 1)
                lefts["X"] = [(c, 0, rest - width) for c in copies]
        for name in "ABD":
            count = groups[name][2]
            res = call_rows(flag, [groups[name]], lefts[name], upper, **solving)
            groups[name] = (res[0], 0, count)
            if k + 1 < K:
                copies = spread(res[1], k + 1)
                lefts[name] = [(c, 0, count) for c in copies]
    first = (row == 0).astype(jnp.int32).reshape(1)
    return fits, finish(put_d, first, [groups["A"][0], groups["B"][0]], groups["D"][0], tops, row_count)


def capacities(n, nr, K):
    unit = n // nr
    cx = up8(1.15 * unit)
    ce = -(-up8(0.36 * unit) // 8) * 8
    return cx, up8(2.5 * unit), ce, up8(0.13 * K * n)


def shards(nr, nc, trailing, pivots, lower_inverse, upper_inverse):
    row_count, col_count = trailing.shape
    K, n = pivots.shape
    fits_shape = (
        K * n < row_count and nr == 8 and nc % 2 == 0 and K <= nc and n == col_count and n % (8 * nr) == 0 and row_count % 16 == 0
    )
    if not fits_shape:
        return plain_steps(trailing, pivots, lower_inverse, upper_inverse, lax.psum)
    caps = CAPS or capacities(n, nr, K)
    fits, done = fast_steps(trailing, pivots, lower_inverse, upper_inverse, nr, nc, caps)
    sizes = {"row": nr, "col": nc}

    def plain(carry):
        total = lambda block, axis: ring_sum(block, axis, sizes[axis])
        return jnp.bool_(False), plain_steps(trailing, pivots, lower_inverse, upper_inverse, total)

    return lax.while_loop(lambda carry: carry[0], plain, (~fits, done))[1]


CAPS = None


def solution(mesh):
    nr, nc = mesh.shape["row"], mesh.shape["col"]
    in_specs = (P("row", "col"), P(), P(), P())
    return jax.shard_map(
        functools.partial(shards, nr, nc), mesh=mesh, in_specs=in_specs, out_specs=P("row", "col"), check_vma=False
    )
```
